32 devices in a mesh: head: 2 (over x), inner: 4 (over y, core), outer: 4 (over z).
Axes of the slice: x: 2, y: 2, z: 4, core: 2. Of those that a mesh axis runs over, the one named last changes fastest.
Arguments:
- queries: float32 [2048, 8, 128], P(('inner', 'outer'), 'head'), may hold values from -8 to 8
- key_rows: float32 [2048, 128], P(('inner', 'outer'), 'head'), may hold values from -8 to 8
- values: float32 [2048, 128], P(('inner', 'outer'), 'head'), may hold values from -24 to 24
- out_grad: float32 [2048, 8, 128], P(('inner', 'outer'), 'head'), may hold values from -48 to 48
- sink_len: int32 [1], replicated, may hold values from 32 to 128
- window_len: int32 [1], replicated, may hold values from 129 to 640
- block_codes: int32 [16, 5], replicated, may hold values from 0 to 2, as said below
Outputs:
- query_grad: float32 [2048, 8, 128], P(('inner', 'outer'), 'head')
- key_grad: float32 [2048, 128], P(('inner', 'outer'), 'head')
- value_grad: float32 [2048, 128], P(('inner', 'outer'), 'head')
The draws below stay inside these ranges and needn't reach their ends.
Inputs may be any that keep to these rules, and one draw needn't show every extreme that they name: block_codes[b, 0] is 1 or 2 for every block b.
All inputs are finite; a program needn't handle non-finite values.
Results may differ from the reference program's by a relative error of at most 0.0003.
Values sent between devices are 32-bit elements; how exact they have to be, the bound alone decides.
A program may use at most 64 MiB of HBM per device.

```python
import math
import jax
import jax.numpy as jnp
from jax import lax

HEAD_DIM = 128
TOK_DEV = 128
STEPS = 5
SINK = 128
NSEQ = 16
TOKENS = 2048
HEADS = 8
KV_HEADS = 1


def paired_draw(key):
    base = jax.random.fold_in(key, 77)
    query_key, key_key = jax.random.split(base, 2)
    queries = jax.random.normal(query_key, (TOKENS, HEADS, HEAD_DIM), jnp.float32)
    key_heads = jax.random.normal(key_key, (TOKENS, KV_HEADS, HEAD_DIM), jnp.float32)
    queries = jnp.clip(queries, -8.0, 8.0)
    key_heads = jnp.clip(key_heads, -8.0, 8.0)
    return (queries, key_heads.reshape(TOKENS, KV_HEADS * HEAD_DIM))


def draw_queries(key, part):
    return paired_draw(key)[0]


def draw_key_rows(key, part):
    return paired_draw(key)[1]


def draw_block_codes(key, part):
    others = jax.random.randint(key, (NSEQ, STEPS), 0, 3, dtype=jnp.int32)
    leading = jax.random.randint(jax.random.fold_in(key, 5), (NSEQ, 1), 1, 3, dtype=jnp.int32)
    return jnp.concatenate([leading, others[:, 1:]], axis=1)


def block_levels(own_key, shape, shards, smallest, high):
    gain, own = 1.0, jax.random.fold_in(own_key, 6)
    for position, blocks in shards:
        steps = jnp.exp(jax.random.uniform(jax.random.fold_in(own, position), (blocks,), jnp.float32, smallest / len(shards), high / len(shards)))
        gain = gain * jnp.repeat(steps, shape[position] // blocks).reshape([-1 if axis == position else 1 for axis in range(len(shape))])
    return gain


def bell_draw(key, shape, width, most, shards=(), kind=jnp.bfloat16):
    result = width * jax.random.normal(key, shape, jnp.float32)
    if shards:
        result = result * block_levels(key, shape, shards, -0.22, 0.18)
    return jnp.clip(result, -most, most).astype(kind)


def setup_inputs(seed: int = 0) -> dict:
    seeds = jax.random.split(jax.random.key(seed), 8)
    return {
        "queries": draw_queries(jax.random.fold_in(seeds[7], 71), 0),
        "key_rows": draw_key_rows(jax.random.fold_in(seeds[7], 71), 0),
        "values": bell_draw(seeds[2], (TOKENS, KV_HEADS * HEAD_DIM), 4.0, 24.0, ((0, 16), (1, 2)), jnp.float32),
        "out_grad": bell_draw(seeds[3], (TOKENS, HEADS, HEAD_DIM), 8.0, 48.0, ((0, 16), (1, 2)), jnp.float32),
        "sink_len": jax.random.randint(seeds[4], (1,), SINK // 4, SINK + 1).astype(jnp.int32),
        "window_len": jax.random.randint(seeds[5], (1,), TOK_DEV + 1, STEPS * TOK_DEV + 1).astype(jnp.int32),
        "block_codes": draw_block_codes(jax.random.fold_in(seeds[7], 71), 0),
    }


very_low = -1e+30
precise = lax.Precision.HIGHEST

def reference(queries, key_rows, values, out_grad, sink_len, window_len, block_codes):
    group = HEADS // KV_HEADS
    temper = 1.0 / math.sqrt(HEAD_DIM)
    front_pad = (STEPS - 1) * TOK_DEV
    span = STEPS * TOK_DEV
    key_heads = key_rows.reshape(TOKENS, KV_HEADS, HEAD_DIM)
    value_heads = values.reshape(TOKENS, KV_HEADS, HEAD_DIM)
    padding = jnp.zeros((front_pad, KV_HEADS, HEAD_DIM), key_rows.dtype)
    padded_keys = jnp.concatenate([padding, key_heads], 0)
    padded_values = jnp.concatenate([padding, value_heads], 0)
    sink_keys = key_heads[:SINK]
    sink_values = value_heads[:SINK]
    sink_end = sink_len[0]
    window = window_len[0]
    local_ids = jnp.arange(TOK_DEV, dtype=jnp.int32)
    spread = jnp.arange(span, dtype=jnp.int32)
    sink_ids = jnp.arange(SINK, dtype=jnp.int32)

    def one_block(carry, query_block):
        grad_keys, grad_values, sink_dk, sink_dv = carry
        start = (query_block * TOK_DEV).astype(jnp.int32)
        query_blk = lax.dynamic_slice_in_dim(queries, start, TOK_DEV, 0).reshape(TOK_DEV, KV_HEADS, group, HEAD_DIM)
        grad_blk = lax.dynamic_slice_in_dim(out_grad, start, TOK_DEV, 0).reshape(TOK_DEV, KV_HEADS, group, HEAD_DIM)
        window_keys = lax.dynamic_slice_in_dim(padded_keys, start, span, 0)
        window_values = lax.dynamic_slice_in_dim(padded_values, start, span, 0)
        all_keys = jnp.concatenate([sink_keys, window_keys], 0)
        all_values = jnp.concatenate([sink_values, window_values], 0)
        pos_q = start + local_ids
        pos_k = start - front_pad + spread
        offsets = (STEPS - 1 - spread // TOK_DEV).astype(jnp.int32)
        code_row = lax.dynamic_index_in_dim(block_codes, query_block, 0, keepdims=False)
        codes = code_row[offsets]
        rule = (codes != 0)[None, :] & ((codes == 2)[None, :] | (pos_q[:, None] - pos_k[None, :] < window))
        in_sink = (pos_k < sink_end)[None, :]
        chosen = jnp.where(query_block == 0, in_sink | rule, jnp.logical_not(in_sink) & rule)
        seen_window = (pos_k >= 0)[None, :] & (pos_k[None, :] <= pos_q[:, None]) & chosen
        seen_sink = jnp.broadcast_to(((query_block >= 1) & (sink_ids < sink_end))[None, :], (TOK_DEV, SINK))
        allowed = jnp.concatenate([seen_sink, seen_window], 1)
        logits = temper * jnp.einsum('tkgd,skd->kgts', query_blk, all_keys, precision=precise)
        logits = jnp.where(allowed, logits, very_low)
        row_max = lax.optimization_barrier(jnp.max(logits, axis=3, keepdims=True))
        weights = jnp.where(allowed, jnp.exp(logits - row_max), 0.0)
        probs = weights / lax.optimization_barrier(jnp.sum(weights, axis=3, keepdims=True))
        attended = jnp.einsum('kgts,skd->tkgd', probs, all_values, precision=precise)
        row_delta = jnp.einsum('tkgd,tkgd->kgt', grad_blk, attended, precision=precise)
        grad_dots = jnp.einsum('tkgd,skd->kgts', grad_blk, all_values, precision=precise)
        dscores = probs * (grad_dots - row_delta[..., None])
        step_dq = temper * jnp.einsum('kgts,skd->tkgd', dscores, all_keys, precision=precise)
        step_dk = temper * jnp.einsum('kgts,tkgd->skd', dscores, query_blk, precision=precise)
        step_dv = jnp.einsum('kgts,tkgd->skd', probs, grad_blk, precision=precise)
        current_k = lax.dynamic_slice_in_dim(grad_keys, start, span, 0)
        grad_keys = lax.dynamic_update_slice_in_dim(grad_keys, current_k + step_dk[SINK:], start, 0)
        current_v = lax.dynamic_slice_in_dim(grad_values, start, span, 0)
        grad_values = lax.dynamic_update_slice_in_dim(grad_values, current_v + step_dv[SINK:], start, 0)
        sink_dk = sink_dk + step_dk[:SINK]
        sink_dv = sink_dv + step_dv[:SINK]
        return ((grad_keys, grad_values, sink_dk, sink_dv), step_dq.reshape(TOK_DEV, HEADS, HEAD_DIM))
    zero_grads = jnp.zeros((front_pad + TOKENS, KV_HEADS, HEAD_DIM), queries.dtype)
    zero_sink = jnp.zeros((SINK, KV_HEADS, HEAD_DIM), queries.dtype)
    carry, stacked = lax.scan(one_block, (zero_grads, zero_grads, zero_sink, zero_sink), jnp.arange(NSEQ, dtype=jnp.int32))
    grad_keys, grad_values, sink_dk, sink_dv = carry
    key_grad = grad_keys[front_pad:].at[:SINK].add(sink_dk)
    value_grad = grad_values[front_pad:].at[:SINK].add(sink_dv)
    query_grad = stacked.reshape(TOKENS, HEADS, HEAD_DIM)
    return (query_grad, key_grad.reshape(TOKENS, KV_HEADS * HEAD_DIM), value_grad.reshape(TOKENS, KV_HEADS * HEAD_DIM))
```

```python
import functools
import math

import jax
import jax.numpy as jnp
from jax import lax
from jax.experimental import pallas as pl
from jax.experimental.pallas import tpu as pltpu
from jax.sharding import PartitionSpec as P

STEPS = 5
FAR = STEPS - 1
BIG = 1 << 28
very_low = -1e30
f32, bf16 = jnp.float32, jnp.bfloat16
MESH = pl.DeviceIdType.MESH
NT = (((1,), (1,)), ((), ()))
NN = (((1,), (0,)), ((), ()))


def dot(a, b, dims):
    return lax.dot_general(a, b, dims, preferred_element_type=f32)


def two(x):
    hi = x.astype(bf16)
    return hi, (x - hi.astype(f32)).astype(bf16)


def three(x):
    hi = x.astype(bf16)
    rest = x - hi.astype(f32)
    mid = rest.astype(bf16)
    return hi, mid, (rest - mid.astype(f32)).astype(bf16)


def kernel(
    sizes, sink_ref, window_ref, codes_ref, q_ref, k_ref, v_ref, g_ref, dq_ref, dk_ref, dv_ref,
    buf, sinkb, piece, qcat, gcat, st, dp, dshi, dslo, ktcat,
    xout, xin, mine, gout, gin, g4out, g4in, sg, sin, s2, s2in, s3, s3in, send, recv,
):
    ni, no, heads_dev = sizes
    block, half = k_ref.shape
    rows = q_ref.shape[0]
    temper = 1.0 / math.sqrt(2 * half)
    head, inner, outer = lax.axis_index("head"), lax.axis_index("inner"), lax.axis_index("outer")
    par = lax.rem(head, 2)
    other = 1 - par
    partner = head + 1 - 2 * par
    count = ni * no
    b = inner * no + outer
    pr = block // ni

    def seq(o):
        t = lax.rem(b + o + count, count)
        return (head, t // no, lax.rem(t, no))

    across = (partner, inner, outer)
    columns = [(p, d) for p in range(2) for d in range(ni) if p or d]

    def column(p, d):
        return (partner if p else head, lax.rem(inner + d, ni), outer)

    def source(d):
        return lax.rem(inner - d + ni, ni)

    slots = {}

    def sem(name):
        return slots.setdefault(name, len(slots))

    pending = []

    def copy(name, src, dst, device):
        k = sem(name)
        return pltpu.make_async_remote_copy(
            src_ref=src, dst_ref=dst, send_sem=send.at[k], recv_sem=recv.at[k],
            device_id=device, device_id_type=MESH,
        )

    def start(name, src, dst, device):
        c = copy(name, src, dst, device)
        c.start()
        pending.append(c)

    def arrived(name, dst):
        copy(name, dst, dst, across).wait_recv()

    buf[0, par, :, 0:half] = k_ref[...]
    buf[0, par, :, half:2 * half] = v_ref[...]

    barrier = pltpu.get_barrier_semaphore()
    greet = [seq(s * o) for o in range(1, STEPS) for s in (1, -1)]
    greet += [column(p, d) for p, d in columns]
    greet += [(head, inner, lax.rem(outer + d, no)) for d in range(1, no)]
    for device in greet:
        pl.semaphore_signal(barrier, inc=1, device_id=device, device_id_type=MESH)

    q0, q1, q2 = three(q_ref[...])
    qcat[...] = jnp.concatenate([q0, q1, q0, q1, q2, q0], 1)
    g0, g1, g2 = three(g_ref[...])
    gcat[...] = jnp.concatenate([g0, g1, g0, g1, g2, g0], 1)
    pl.semaphore_wait(barrier, len(greet))

    own = buf.at[0, par]
    first = (inner == 0) & (outer == 0)
    top = outer == 0
    at_root = piece

    @pl.when(first)
    def _():
        for i in range(1, ni):
            copy(f"f1_{i}", own.at[pl.ds(i * pr, pr)], at_root, (head, i, outer)).start()
        piece[...] = buf[0, par, 0:pr, :]

    start("x0", own, own, across)
    for o in range(FAR, 0, -1):
        start(f"w{o}", own, buf.at[o, par], seq(o))

    def scores_of(a, c, index, allowed):
        lane = lax.broadcasted_iota(jnp.int32, (block, 2 * half), 1)
        low = lane < half
        keys = jnp.where(low, a, pltpu.roll(c, half, 1))
        vals = jnp.where(low, pltpu.roll(a, half, 1), c)
        k0, k1, k2 = three(keys)
        v0, v1, v2 = three(vals)
        s = dot(jnp.concatenate([k0, k0, k1, k1, k0, k2], 1), qcat[...], NT)
        st[index] = jnp.where(allowed, temper * s, very_low)
        dp[index] = dot(jnp.concatenate([v0, v0, v1, v1, v0, v2], 1), gcat[...], NT)
        t0, t1 = two(keys.T * temper)
        ktcat[index] = jnp.concatenate([t0, t1, t0], 1)

    jk = lax.broadcasted_iota(jnp.int32, (block, rows), 0)
    iq = lax.broadcasted_iota(jnp.int32, (block, rows), 1) // heads_dev
    gap = iq - jk
    sink_end, window = sink_ref[0], window_ref[0]

    def mask_of(o):
        code = codes_ref[b, o]
        limit = jnp.where(code == 2, BIG, jnp.where(code == 1, window, -BIG))
        limit = jnp.where(b >= o, limit, -BIG) - o * block
        here = jnp.where(b == o, sink_end, 0)
        if o == 0:
            return (gap >= 0) & ((gap < limit) | (jk < here))
        return (gap < limit) & (jk >= here)

    def slot(o):
        scores_of(buf[o, 0], buf[o, 1], o, mask_of(o))

    arrived("x0", buf.at[0, other])
    start("w4x", buf.at[0, other], buf.at[FAR, other], seq(FAR))

    @pl.when(top)
    def _():
        @pl.when(inner != 0)
        def _():
            for i in range(1, ni):
                @pl.when(inner == i)
                def _():
                    arrived(f"f1_{i}", piece)
        for z in range(1, no):
            copy(f"f2_{z}", piece, piece, (head, inner, z)).start()

    slot(0)
    for o in range(1, FAR):
        arrived(f"w{o}", buf.at[o, par])
        start(f"r{o}", buf.at[o, par], buf.at[o, par], across)

    @pl.when(outer != 0)
    def _():
        for z in range(1, no):
            @pl.when(outer == z)
            def _():
                arrived(f"f2_{z}", piece)

    where = pl.ds(pl.multiple_of(inner * pr, pr), pr)
    for p, d in columns:
        start(f"f3_{p}_{d}", piece, sinkb.at[par, where], column(p, d))
    sinkb[par, where] = piece[...]

    arrived(f"w{FAR}", buf.at[FAR, par])
    arrived("w4x", buf.at[FAR, other])
    slot(FAR)
    for o in range(1, FAR):
        arrived(f"r{o}", buf.at[o, other])
        slot(o)
    for p, d in columns:
        there = pl.ds(pl.multiple_of(source(d) * pr, pr), pr)
        arrived(f"f3_{p}_{d}", sinkb.at[other if p else par, there])
    scores_of(sinkb[0], sinkb[1], STEPS, jk < jnp.where(b >= 1, sink_end, 0))

    total = STEPS + 1
    top_score = jnp.max(st[0], axis=0, keepdims=True)
    for i in range(1, total):
        top_score = jnp.maximum(top_score, jnp.max(st[i], axis=0, keepdims=True))
    norm = jnp.zeros((1, rows), f32)
    delta = jnp.zeros((1, rows), f32)
    for i in range(total):
        e = jnp.exp(st[i] - top_score)
        st[i] = e
        norm = norm + jnp.sum(e, axis=0, keepdims=True)
        delta = delta + jnp.sum(e * dp[i], axis=0, keepdims=True)
    scale = 1.0 / norm
    delta = delta * scale

    def grads(i):
        probs = st[i] * scale
        ds = probs * (dp[i] - delta)
        p_hi, p_lo = two(probs)
        d_hi, d_lo = two(ds)
        dshi[i] = d_hi
        dslo[i] = d_lo
        w = 2 * half
        pv = dot(p_hi, gcat[:, 0:2 * w], NN)
        dv = pv[:, 0:w] + pv[:, w:] + dot(p_lo, gcat[:, 0:w], NN)
        kq = dot(d_hi, qcat[:, 0:2 * w], NN)
        dk = temper * (kq[:, 0:w] + kq[:, w:] + dot(d_lo, qcat[:, 0:w], NN))
        low = lax.broadcasted_iota(jnp.int32, (block, w), 1) < half
        even = jnp.where(low, dk, pltpu.roll(dv, half, 1))
        odd = jnp.where(low, pltpu.roll(dk, half, 1), dv)
        keep = jnp.where(par == 0, even, odd)
        give = jnp.where(par == 0, odd, even)
        return keep, give

    keep, give = grads(STEPS)
    sg[0] = keep
    sg[1] = give
    for p, d in columns:
        target = lax.rem(inner + d, ni)
        rng = pl.ds(pl.multiple_of(target * pr, pr), pr)
        start(f"b1_{p}_{d}", sg.at[p, rng], sin.at[p * ni + d], column(p, d))

    keep, give = grads(FAR)
    g4out[0] = keep
    g4out[1] = give
    start("g4k", g4out.at[0], g4in.at[0], seq(-FAR))
    start("g4g", g4out.at[1], g4in.at[1], seq(-FAR))

    def pass_on(o):
        arrived(f"gx{o}", xin.at[o])
        gout[o] = mine[o] + xin[o]
        start(f"gz{o}", gout.at[o], gin.at[o], seq(-o))

    for o in range(FAR - 1, 0, -1):
        keep, give = grads(o)
        mine[o] = keep
        xout[o] = give
        start(f"gx{o}", xout.at[o], xin.at[o], across)
        if o < FAR - 1:
            pass_on(o + 1)
    keep, give = grads(0)
    arrived("g4g", g4in.at[1])
    xout[0] = give + g4in[1]
    start("gx0", xout.at[0], xin.at[0], across)
    pass_on(1)
    arrived("g4k", g4in.at[0])
    mine[0] = keep + g4in[0]

    for p, d in columns:
        arrived(f"b1_{p}_{d}", sin.at[p * ni + d])
    acc = sg[0, where]
    for p, d in columns:
        acc = acc + sin[p * ni + d]
    s2[...] = acc
    for z in range(1, no):
        @pl.when(outer == z)
        def _():
            copy(f"b2_{z}", s2, s2in.at[z], (head, inner, 0)).start()

    dqt = jnp.zeros((2 * half, rows), f32)
    for i in range(total):
        hi = dshi[i]
        dqt = dqt + dot(ktcat[i], jnp.concatenate([hi, hi, dslo[i]], 0), NN)
    dq_ref[...] = dqt.T

    @pl.when(top)
    def _():
        part = s2[...]
        for z in range(1, no):
            arrived(f"b2_{z}", s2in.at[z])
            part = part + s2in[z]
        s3[...] = part
        for i in range(1, ni):
            @pl.when(inner == i)
            def _():
                copy(f"b3_{i}", s3, s3in.at[i], (head, 0, outer)).start()

    arrived("gx0", xin.at[0])
    acc = mine[0] + xin[0]
    for o in range(FAR - 1, 0, -1):
        arrived(f"gz{o}", gin.at[o])
        acc = acc + gin[o]
    mine[0] = acc

    @pl.when(first)
    def _():
        mine[0, 0:pr] += s3[...]
        for i in range(1, ni):
            arrived(f"b3_{i}", s3in.at[i])
            mine[0, i * pr:(i + 1) * pr] += s3in[i]

    acc = mine[0]
    dk_ref[...] = acc[:, 0:half]
    dv_ref[...] = acc[:, half:]

    for c in pending:
        c.wait_send()

    @pl.when(first)
    def _():
        for i in range(1, ni):
            copy(f"f1_{i}", own.at[pl.ds(i * pr, pr)], at_root, (head, i, outer)).wait_send()

    @pl.when(top)
    def _():
        for z in range(1, no):
            copy(f"f2_{z}", piece, piece, (head, inner, z)).wait_send()
        for i in range(1, ni):
            @pl.when(inner == i)
            def _():
                copy(f"b3_{i}", s3, s3in.at[i], (head, 0, outer)).wait_send()

    for z in range(1, no):
        @pl.when(outer == z)
        def _():
            copy(f"b2_{z}", s2, s2in.at[z], (head, inner, 0)).wait_send()
    assert len(slots) <= send.shape[0]


def shards(ni, no, queries, key_rows, values, out_grad, sink_len, window_len, block_codes):
    block, heads_dev, dim = queries.shape
    rows = block * heads_dev
    half = key_rows.shape[1]
    pr = block // ni
    total = STEPS + 1
    sems = 2 * (ni - 1) + 2 * (no - 1) + 2 * (2 * ni - 1) + 4 * STEPS
    vmem, smem = pl.BlockSpec(memory_space=pltpu.VMEM), pl.BlockSpec(memory_space=pltpu.SMEM)
    tile = (block, dim)
    grad_q, grad_k, grad_v = pl.pallas_call(
        functools.partial(kernel, (ni, no, heads_dev)),
        out_shape=(
            jax.ShapeDtypeStruct((rows, dim), f32),
            jax.ShapeDtypeStruct((block, half), f32),
            jax.ShapeDtypeStruct((block, half), f32),
        ),
        in_specs=[smem] * 3 + [vmem] * 4,
        out_specs=(vmem,) * 3,
        scratch_shapes=[
            pltpu.VMEM((STEPS, 2) + tile, f32),
            pltpu.VMEM((2,) + tile, f32),
            pltpu.VMEM((pr, dim), f32),
            pltpu.VMEM((rows, 6 * dim), bf16),
            pltpu.VMEM((rows, 6 * dim), bf16),
            pltpu.VMEM((total, block, rows), f32),
            pltpu.VMEM((total, block, rows), f32),
            pltpu.VMEM((total, block, rows), bf16),
            pltpu.VMEM((total, block, rows), bf16),
            pltpu.VMEM((total, dim, 3 * block), bf16),
            pltpu.VMEM((FAR,) + tile, f32),
            pltpu.VMEM((FAR,) + tile, f32),
            pltpu.VMEM((FAR,) + tile, f32),
            pltpu.VMEM((FAR,) + tile, f32),
            pltpu.VMEM((FAR,) + tile, f32),
            pltpu.VMEM((2,) + tile, f32),
            pltpu.VMEM((2,) + tile, f32),
            pltpu.VMEM((2,) + tile, f32),
            pltpu.VMEM((2 * ni, pr, dim), f32),
            pltpu.VMEM((pr, dim), f32),
            pltpu.VMEM((no, pr, dim), f32),
            pltpu.VMEM((pr, dim), f32),
            pltpu.VMEM((ni, pr, dim), f32),
            pltpu.SemaphoreType.DMA((sems,)),
            pltpu.SemaphoreType.DMA((sems,)),
        ],
        compiler_params=pltpu.CompilerParams(
            collective_id=0, has_side_effects=True, vmem_limit_bytes=48 << 20
        ),
    )(
        sink_len, window_len, block_codes,
        queries.reshape(rows, dim), key_rows, values, out_grad.reshape(rows, dim),
    )
    return grad_q.reshape(queries.shape), grad_k, grad_v


def solution(mesh):
    in_specs = (
        P(("inner", "outer"), "head", None),
        P(("inner", "outer"), "head"),
        P(("inner", "outer"), "head"),
        P(("inner", "outer"), "head", None),
        P(),
        P(),
        P(),
    )
    out_specs = (
        P(("inner", "outer"), "head", None),
        P(("inner", "outer"), "head"),
        P(("inner", "outer"), "head"),
    )
    body = functools.partial(shards, mesh.shape["inner"], mesh.shape["outer"])
    return jax.shard_map(body, mesh=mesh, in_specs=in_specs, out_specs=out_specs, check_vma=False)
```

```python
import functools
import math

import jax
import jax.numpy as jnp
from jax import lax
from jax.experimental import pallas as pl
from jax.experimental.pallas import tpu as pltpu
from jax.sharding import PartitionSpec as P

STEPS = 5
FAR = STEPS - 1
BIG = 1 << 28
very_low = -1e30
f32, bf16 = jnp.float32, jnp.bfloat16
MESH = pl.DeviceIdType.MESH
NT = (((1,), (1,)), ((), ()))
NN = (((1,), (0,)), ((), ()))


def dot(a, b, dims):
    return lax.dot_general(a, b, dims, preferred_element_type=f32)


def two(x):
    hi = x.astype(bf16)
    return hi, (x - hi.astype(f32)).astype(bf16)


def three(x):
    hi = x.astype(bf16)
    rest = x - hi.astype(f32)
    mid = rest.astype(bf16)
    return hi, mid, (rest - mid.astype(f32)).astype(bf16)


def kernel(
    sizes, sink_ref, window_ref, codes_hbm, q_hbm, k_hbm, v_hbm, g_hbm, dq_ref, dkv_ref,
    codes_ref, q_ref, g_ref, load, buf, sinkb, piece, qcat, gcat, st, dp, dshi, dslo, ktcat,
    xout, xin, mine, gout, gin, g4out, g4in, sg, sin, s2, s2in, s3, s3in, send, recv,
):
    ni, no, heads_dev = sizes
    half, block = k_hbm.shape
    rows = q_ref.shape[0]
    temper = 1.0 / math.sqrt(2 * half)
    head, inner, outer = lax.axis_index("head"), lax.axis_index("inner"), lax.axis_index("outer")
    par = lax.rem(head, 2)
    other = 1 - par
    partner = head + 1 - 2 * par
    count = ni * no
    b = inner * no + outer
    pr = block // ni

    def seq(o):
        t = lax.rem(b + o + count, count)
        return (head, t // no, lax.rem(t, no))

    across = (partner, inner, outer)
    columns = [(p, d) for p in range(2) for d in range(ni) if p or d]

    def column(p, d):
        return (partner if p else head, lax.rem(inner + d, ni), outer)

    def source(d):
        return lax.rem(inner - d + ni, ni)

    slots = {}

    def sem(name):
        return slots.setdefault(name, len(slots))

    pending = []

    def copy(name, src, dst, device):
        k = sem(name)
        return pltpu.make_async_remote_copy(
            src_ref=src, dst_ref=dst, send_sem=send.at[k], recv_sem=recv.at[k],
            device_id=device, device_id_type=MESH,
        )

    def start(name, src, dst, device):
        c = copy(name, src, dst, device)
        c.start()
        pending.append(c)

    def arrived(name, dst):
        copy(name, dst, dst, across).wait_recv()

    moves = [
        (k_hbm, buf.at[0, par, 0:half]), (v_hbm, buf.at[0, par, half:2 * half]),
        (q_hbm, q_ref), (g_hbm, g_ref),
        (codes_hbm, codes_ref),
    ]
    loads = [pltpu.make_async_copy(x, y, load.at[i]) for i, (x, y) in enumerate(moves)]
    for x in loads:
        x.start()

    barrier = pltpu.get_barrier_semaphore()
    greet = [seq(s * o) for o in range(1, STEPS) for s in (1, -1)]
    greet += [column(p, d) for p, d in columns]
    greet += [(head, inner, lax.rem(outer + d, no)) for d in range(1, no)]
    for device in greet:
        pl.semaphore_signal(barrier, inc=1, device_id=device, device_id_type=MESH)

    for x in loads:
        x.wait()
    q0, q1, q2 = three(q_ref[...])
    qcat[...] = jnp.concatenate([q0, q1, q0, q1, q2, q0], 1)
    g0, g1, g2 = three(g_ref[...])
    gcat[...] = jnp.concatenate([g0, g1, g0, g1, g2, g0], 1)
    pl.semaphore_wait(barrier, len(greet))

    own = buf.at[0, par]
    first = (inner == 0) & (outer == 0)
    top = outer == 0
    at_root = piece

    @pl.when(first)
    def _():
        for i in range(1, ni):
            copy(f"f1_{i}", own.at[pl.ds(i * pr, pr)], at_root, (head, i, outer)).start()
        piece[...] = buf[0, par, 0:pr, :]

    start("x0", own, own, across)
    for o in range(FAR, 0, -1):
        start(f"w{o}", own, buf.at[o, par], seq(o))

    def scores_of(a, c, index, allowed):
        keys = jnp.concatenate([a[0:half], c[0:half]], 0)
        vals = jnp.concatenate([a[half:], c[half:]], 0)
        k0, k1, k2 = three(keys.T)
        v0, v1, v2 = three(vals.T)
        s = dot(jnp.concatenate([k0, k0, k1, k1, k0, k2], 1), qcat[...], NT)
        st[index] = jnp.where(allowed, temper * s, very_low)
        dp[index] = dot(jnp.concatenate([v0, v0, v1, v1, v0, v2], 1), gcat[...], NT)
        t0, t1 = two(keys * temper)
        ktcat[index] = jnp.concatenate([t0, t1, t0], 1)

    jk = lax.broadcasted_iota(jnp.int32, (block, rows), 0)
    iq = lax.broadcasted_iota(jnp.int32, (block, rows), 1) // heads_dev
    gap = iq - jk
    sink_end, window = sink_ref[0], window_ref[0]

    def mask_of(o):
        code = codes_ref[o, b]
        limit = jnp.where(code == 2, BIG, jnp.where(code == 1, window, -BIG))
        limit = jnp.where(b >= o, limit, -BIG) - o * block
        here = jnp.where(b == o, sink_end, 0)
        if o == 0:
            return (gap >= 0) & ((gap < limit) | (jk < here))
        return (gap < limit) & (jk >= here)

    def slot(o):
        scores_of(buf[o, 0], buf[o, 1], o, mask_of(o))

    arrived("x0", buf.at[0, other])
    start("w4x", buf.at[0, other], buf.at[FAR, other], seq(FAR))

    @pl.when(top)
    def _():
        @pl.when(inner != 0)
        def _():
            for i in range(1, ni):
                @pl.when(inner == i)
                def _():
                    arrived(f"f1_{i}", piece)
        for z in range(1, no):
            copy(f"f2_{z}", piece, piece, (head, inner, z)).start()

    slot(0)
    for o in range(1, FAR):
        arrived(f"w{o}", buf.at[o, par])
        start(f"r{o}", buf.at[o, par], buf.at[o, par], across)

    @pl.when(outer != 0)
    def _():
        for z in range(1, no):
            @pl.when(outer == z)
            def _():
                arrived(f"f2_{z}", piece)

    where = pl.ds(pl.multiple_of(inner * pr, pr), pr)
    for p, d in columns:
        start(f"f3_{p}_{d}", piece, sinkb.at[par, where], column(p, d))
    sinkb[par, where] = piece[...]

    arrived(f"w{FAR}", buf.at[FAR, par])
    arrived("w4x", buf.at[FAR, other])
    slot(FAR)
    for o in range(1, FAR):
        arrived(f"r{o}", buf.at[o, other])
        slot(o)
    for p, d in columns:
        there = pl.ds(pl.multiple_of(source(d) * pr, pr), pr)
        arrived(f"f3_{p}_{d}", sinkb.at[other if p else par, there])
    scores_of(sinkb[0], sinkb[1], STEPS, jk < jnp.where(b >= 1, sink_end, 0))

    total = STEPS + 1
    top_score = jnp.max(st[0], axis=0, keepdims=True)
    for i in range(1, total):
        top_score = jnp.maximum(top_score, jnp.max(st[i], axis=0, keepdims=True))
    norm = jnp.zeros((1, rows), f32)
    delta = jnp.zeros((1, rows), f32)
    for i in range(total):
        e = jnp.exp(st[i] - top_score)
        st[i] = e
        norm = norm + jnp.sum(e, axis=0, keepdims=True)
        delta = delta + jnp.sum(e * dp[i], axis=0, keepdims=True)
    scale = 1.0 / norm
    delta = delta * scale

    def grads(i):
        probs = st[i] * scale
        ds = probs * (dp[i] - delta)
        p_hi, p_lo = two(probs)
        d_hi, d_lo = two(ds)
        dshi[i] = d_hi
        dslo[i] = d_lo
        w = 2 * half
        pv = dot(p_hi, gcat[:, 0:2 * w], NN)
        dv = pv[:, 0:w] + pv[:, w:] + dot(p_lo, gcat[:, 0:w], NN)
        kq = dot(d_hi, qcat[:, 0:2 * w], NN)
        dk = temper * (kq[:, 0:w] + kq[:, w:] + dot(d_lo, qcat[:, 0:w], NN))
        dk, dv = dk.T, dv.T
        even = jnp.concatenate([dk[0:half], dv[0:half]], 0)
        odd = jnp.concatenate([dk[half:], dv[half:]], 0)
        keep = jnp.where(par == 0, even, odd)
        give = jnp.where(par == 0, odd, even)
        return keep, give

    keep, give = grads(STEPS)
    sg[0] = keep
    sg[1] = give
    for p, d in columns:
        target = lax.rem(inner + d, ni)
        rng = pl.ds(pl.multiple_of(target * pr, pr), pr)
        start(f"b1_{p}_{d}", sg.at[p, rng], sin.at[p * ni + d], column(p, d))

    keep, give = grads(FAR)
    g4out[0] = keep
    g4out[1] = give
    start("g4k", g4out.at[0], g4in.at[0], seq(-FAR))
    start("g4g", g4out.at[1], g4in.at[1], seq(-FAR))

    def pass_on(o):
        arrived(f"gx{o}", xin.at[o])
        gout[o] = mine[o] + xin[o]
        start(f"gz{o}", gout.at[o], gin.at[o], seq(-o))

    for o in range(FAR - 1, 0, -1):
        keep, give = grads(o)
        mine[o] = keep
        xout[o] = give
        start(f"gx{o}", xout.at[o], xin.at[o], across)
        if o < FAR - 1:
            pass_on(o + 1)
    for p, d in columns:
        arrived(f"b1_{p}_{d}", sin.at[p * ni + d])
    acc = sg[0, where]
    for p, d in columns:
        acc = acc + sin[p * ni + d]
    s2[...] = acc
    for z in range(1, no):
        @pl.when(outer == z)
        def _():
            copy(f"b2_{z}", s2, s2in.at[z], (head, inner, 0)).start()

    keep, give = grads(0)
    arrived("g4g", g4in.at[1])
    xout[0] = give + g4in[1]
    start("gx0", xout.at[0], xin.at[0], across)
    pass_on(1)
    arrived("g4k", g4in.at[0])
    mine[0] = keep + g4in[0]

    dqt = jnp.zeros((2 * half, rows), f32)
    for i in range(total):
        hi = dshi[i]
        dqt = dqt + dot(ktcat[i], jnp.concatenate([hi, hi, dslo[i]], 0), NN)
    dq_ref[...] = dqt.T

    @pl.when(top)
    def _():
        part = s2[...]
        for z in range(1, no):
            arrived(f"b2_{z}", s2in.at[z])
            part = part + s2in[z]
        s3[...] = part
        for i in range(1, ni):
            @pl.when(inner == i)
            def _():
                copy(f"b3_{i}", s3, s3in.at[i], (head, 0, outer)).start()

    arrived("gx0", xin.at[0])
    acc = mine[0] + xin[0]
    for o in range(FAR - 1, 0, -1):
        arrived(f"gz{o}", gin.at[o])
        acc = acc + gin[o]
    mine[0] = acc

    @pl.when(first)
    def _():
        mine[0, 0:pr] += s3[...]
        for i in range(1, ni):
            arrived(f"b3_{i}", s3in.at[i])
            mine[0, i * pr:(i + 1) * pr] += s3in[i]

    dkv_ref[...] = mine[0]

    for c in pending:
        c.wait_send()

    @pl.when(first)
    def _():
        for i in range(1, ni):
            copy(f"f1_{i}", own.at[pl.ds(i * pr, pr)], at_root, (head, i, outer)).wait_send()

    @pl.when(top)
    def _():
        for z in range(1, no):
            copy(f"f2_{z}", piece, piece, (head, inner, z)).wait_send()
        for i in range(1, ni):
            @pl.when(inner == i)
            def _():
                copy(f"b3_{i}", s3, s3in.at[i], (head, 0, outer)).wait_send()

    for z in range(1, no):
        @pl.when(outer == z)
        def _():
            copy(f"b2_{z}", s2, s2in.at[z], (head, inner, 0)).wait_send()
    assert len(slots) <= send.shape[0]


def store(dq_ref, dkv_ref, dq_hbm, dk_hbm, dv_hbm, sem):
    half = dk_hbm.shape[0]
    moves = [
        (dq_ref, dq_hbm), (dkv_ref.at[0:half], dk_hbm), (dkv_ref.at[half:2 * half], dv_hbm),
    ]
    copies = [pltpu.make_async_copy(x, y, sem.at[i]) for i, (x, y) in enumerate(moves)]
    for c in copies:
        c.start()
    for c in copies:
        c.wait()


def shards(ni, no, queries, key_rows, values, out_grad, sink_len, window_len, block_codes):
    block, heads_dev, dim = queries.shape
    rows = block * heads_dev
    half = key_rows.shape[1]
    codes = block_codes.T
    pr = block // ni
    total = STEPS + 1
    sems = 2 * (ni - 1) + 2 * (no - 1) + 2 * (2 * ni - 1) + 4 * STEPS
    smem = pl.BlockSpec(memory_space=pltpu.SMEM)
    vmem, hbm = pl.BlockSpec(memory_space=pltpu.VMEM), pl.BlockSpec(memory_space=pltpu.HBM)
    tile = (block, dim)
    grad_q, grad_kv = pl.pallas_call(
        functools.partial(kernel, (ni, no, heads_dev)),
        out_shape=(
            pltpu.VMEM((rows, dim), f32),
            pltpu.VMEM((2 * half, block), f32),
        ),
        in_specs=[smem] * 2 + [hbm] * 5,
        out_specs=(vmem,) * 2,
        scratch_shapes=[
            pltpu.SMEM(codes.shape, jnp.int32),
            pltpu.VMEM((rows, dim), f32),
            pltpu.VMEM((rows, dim), f32),
            pltpu.SemaphoreType.DMA((5,)),
            pltpu.VMEM((STEPS, 2) + tile, f32),
            pltpu.VMEM((2,) + tile, f32),
            pltpu.VMEM((pr, dim), f32),
            pltpu.VMEM((rows, 6 * dim), bf16),
            pltpu.VMEM((rows, 6 * dim), bf16),
            pltpu.VMEM((total, block, rows), f32),
            pltpu.VMEM((total, block, rows), f32),
            pltpu.VMEM((total, block, rows), bf16),
            pltpu.VMEM((total, block, rows), bf16),
            pltpu.VMEM((total, dim, 3 * block), bf16),
            pltpu.VMEM((FAR,) + tile, f32),
            pltpu.VMEM((FAR,) + tile, f32),
            pltpu.VMEM((FAR,) + tile, f32),
            pltpu.VMEM((FAR,) + tile, f32),
            pltpu.VMEM((FAR,) + tile, f32),
            pltpu.VMEM((2,) + tile, f32),
            pltpu.VMEM((2,) + tile, f32),
            pltpu.VMEM((2,) + tile, f32),
            pltpu.VMEM((2 * ni, pr, dim), f32),
            pltpu.VMEM((pr, dim), f32),
            pltpu.VMEM((no, pr, dim), f32),
            pltpu.VMEM((pr, dim), f32),
            pltpu.VMEM((ni, pr, dim), f32),
            pltpu.SemaphoreType.DMA((sems,)),
            pltpu.SemaphoreType.DMA((sems,)),
        ],
        compiler_params=pltpu.CompilerParams(
            collective_id=0, has_side_effects=True, vmem_limit_bytes=66_000_000
        ),
    )(
        sink_len, window_len, codes,
        queries.reshape(rows, dim), key_rows.T, values.T, out_grad.reshape(rows, dim),
    )
    grad_q, grad_k, grad_v = pl.pallas_call(
        store,
        out_shape=(
            jax.ShapeDtypeStruct((rows, dim), f32),
            jax.ShapeDtypeStruct((half, block), f32),
            jax.ShapeDtypeStruct((half, block), f32),
        ),
        in_specs=[vmem] * 2,
        out_specs=(hbm,) * 3,
        scratch_shapes=[pltpu.SemaphoreType.DMA((3,))],
        compiler_params=pltpu.CompilerParams(vmem_limit_bytes=1 << 20),
    )(grad_q, grad_kv)
    return grad_q.reshape(queries.shape), grad_k.T, grad_v.T


def solution(mesh):
    in_specs = (
        P(("inner", "outer"), "head", None),
        P(("inner", "outer"), "head"),
        P(("inner", "outer"), "head"),
        P(("inner", "outer"), "head", None),
        P(),
        P(),
        P(),
    )
    out_specs = (
        P(("inner", "outer"), "head", None),
        P(("inner", "outer"), "head"),
        P(("inner", "outer"), "head"),
    )
    body = functools.partial(shards, mesh.shape["inner"], mesh.shape["outer"])
    return jax.shard_map(body, mesh=mesh, in_specs=in_specs, out_specs=out_specs, check_vma=False)
```

```python
import functools
import math

import jax
import jax.numpy as jnp
from jax import lax
from jax.experimental import pallas as pl
from jax.experimental.pallas import tpu as pltpu
from jax.sharding import PartitionSpec as P

STEPS = 5
FAR = STEPS - 1
BIG = 1 << 28
very_low = -1e30
f32, bf16 = jnp.float32, jnp.bfloat16
MESH = pl.DeviceIdType.MESH
NT = (((1,), (1,)), ((), ()))
NN = (((1,), (0,)), ((), ()))


def dot(a, b, dims):
    return lax.dot_general(a, b, dims, preferred_element_type=f32)


def two(x):
    hi = x.astype(bf16)
    return hi, (x - hi.astype(f32)).astype(bf16)


def three(x):
    hi = x.astype(bf16)
    rest = x - hi.astype(f32)
    mid = rest.astype(bf16)
    return hi, mid, (rest - mid.astype(f32)).astype(bf16)


def kernel(
    sizes, sink_ref, window_ref, codes_hbm, q_hbm, k_hbm, v_hbm, g_hbm, dq_ref, dkv_ref,
    codes_ref, q_ref, g_ref, load, own, buf, sinkb, piece, qcat, gcat, st, dp, dshi, dslo, ktcat,
    xout, xin, mine, gout, gin, g4out, g4in, fin, sg, sin, s2, s2in, s3, s3in, send, recv,
):
    ni, no, heads_dev = sizes
    half, block = k_hbm.shape
    rows = q_ref.shape[0]
    temper = 1.0 / math.sqrt(2 * half)
    head, inner, outer = lax.axis_index("head"), lax.axis_index("inner"), lax.axis_index("outer")
    par = lax.rem(head, 2)
    other = 1 - par
    partner = head + 1 - 2 * par
    count = ni * no
    b = inner * no + outer
    pr = block // ni

    def seq(o):
        t = lax.rem(b + o + count, count)
        return (head, t // no, lax.rem(t, no))

    across = (partner, inner, outer)
    columns = [(p, d) for p in range(2) for d in range(ni) if p or d]

    def column(p, d):
        return (partner if p else head, lax.rem(inner + d, ni), outer)

    def source(d):
        return lax.rem(inner - d + ni, ni)

    slots = {}

    def sem(name):
        return slots.setdefault(name, len(slots))

    pending = []

    def copy(name, src, dst, device):
        k = sem(name)
        return pltpu.make_async_remote_copy(
            src_ref=src, dst_ref=dst, send_sem=send.at[k], recv_sem=recv.at[k],
            device_id=device, device_id_type=MESH,
        )

    def start(name, src, dst, device):
        c = copy(name, src, dst, device)
        c.start()
        pending.append(c)

    def arrived(name, dst):
        copy(name, dst, dst, across).wait_recv()

    moves = [
        (k_hbm, buf.at[0, 0, par]), (v_hbm, buf.at[1, 0, par]),
        (k_hbm, own.at[0:half]), (v_hbm, own.at[half:2 * half]),
        (q_hbm, q_ref), (g_hbm, g_ref), (codes_hbm, codes_ref),
    ]
    loads = [pltpu.make_async_copy(x, y, load.at[i]) for i, (x, y) in enumerate(moves)]
    for x in loads:
        x.start()

    barrier = pltpu.get_barrier_semaphore()
    greet = [seq(s * o) for o in range(1, STEPS) for s in (1, -1)]
    greet += [column(p, d) for p, d in columns]
    greet += [(head, inner, lax.rem(outer + d, no)) for d in range(1, no)]
    for device in greet:
        pl.semaphore_signal(barrier, inc=1, device_id=device, device_id_type=MESH)

    for x in loads:
        x.wait()
    q0, q1, q2 = three(q_ref[...])
    qcat[...] = jnp.concatenate([q0, q1, q0, q1, q2, q0], 1)
    g0, g1, g2 = three(g_ref[...])
    gcat[...] = jnp.concatenate([g0, g1, g0, g1, g2, g0], 1)
    pl.semaphore_wait(barrier, len(greet))

    first = (inner == 0) & (outer == 0)
    top = outer == 0
    at_root = piece

    @pl.when(first)
    def _():
        for i in range(1, ni):
            copy(f"f1_{i}", own.at[pl.ds(i * pr, pr)], at_root, (head, i, outer)).start()
        piece[...] = own[0:pr, :]

    for kind in range(2):
        mine_kv = buf.at[kind, 0, par]
        start(f"x0{kind}", mine_kv, mine_kv, across)
        for o in range(FAR, 0, -1):
            start(f"w{o}{kind}", mine_kv, buf.at[kind, o, par], seq(o))

    def scores_of(keys, index, allowed):
        k0, k1, k2 = three(keys.T)
        s = dot(jnp.concatenate([k0, k0, k1, k1, k0, k2], 1), qcat[...], NT)
        st[index] = jnp.where(allowed, temper * s, very_low)
        t0, t1 = two(keys * temper)
        ktcat[index] = jnp.concatenate([t0, t1, t0], 1)

    def products_of(vals, index):
        v0, v1, v2 = three(vals.T)
        dp[index] = dot(jnp.concatenate([v0, v0, v1, v1, v0, v2], 1), gcat[...], NT)

    def joined(kind, o):
        return jnp.concatenate([buf[kind, o, 0], buf[kind, o, 1]], 0)

    jk = lax.broadcasted_iota(jnp.int32, (block, rows), 0)
    iq = lax.broadcasted_iota(jnp.int32, (block, rows), 1) // heads_dev
    gap = iq - jk
    sink_end, window = sink_ref[0], window_ref[0]

    def mask_of(o):
        code = codes_ref[o, b]
        limit = jnp.where(code == 2, BIG, jnp.where(code == 1, window, -BIG))
        limit = jnp.where(b >= o, limit, -BIG) - o * block
        here = jnp.where(b == o, sink_end, 0)
        if o == 0:
            return (gap >= 0) & ((gap < limit) | (jk < here))
        return (gap < limit) & (jk >= here)

    def slot(o):
        scores_of(joined(0, o), o, mask_of(o))

    def far_other(kind):
        arrived(f"x0{kind}", buf.at[kind, 0, other])
        start(f"w4x{kind}", buf.at[kind, 0, other], buf.at[kind, FAR, other], seq(FAR))

    def relay(kind, o):
        arrived(f"w{o}{kind}", buf.at[kind, o, par])
        start(f"r{o}{kind}", buf.at[kind, o, par], buf.at[kind, o, par], across)

    far_other(0)

    @pl.when(top)
    def _():
        @pl.when(inner != 0)
        def _():
            for i in range(1, ni):
                @pl.when(inner == i)
                def _():
                    arrived(f"f1_{i}", piece)
        for z in range(1, no):
            copy(f"f2_{z}", piece, piece, (head, inner, z)).start()

    slot(0)
    for o in range(1, FAR):
        relay(0, o)
    far_other(1)

    @pl.when(outer != 0)
    def _():
        for z in range(1, no):
            @pl.when(outer == z)
            def _():
                arrived(f"f2_{z}", piece)

    where = pl.ds(pl.multiple_of(inner * pr, pr), pr)
    for p, d in columns:
        start(f"f3_{p}_{d}", piece, sinkb.at[par, where], column(p, d))
    sinkb[par, where] = piece[...]

    arrived(f"w{FAR}0", buf.at[0, FAR, par])
    arrived("w4x0", buf.at[0, FAR, other])
    slot(FAR)
    for o in range(1, FAR):
        relay(1, o)
    for o in range(1, FAR):
        arrived(f"r{o}0", buf.at[0, o, other])
        slot(o)
    for p, d in columns:
        there = pl.ds(pl.multiple_of(source(d) * pr, pr), pr)
        arrived(f"f3_{p}_{d}", sinkb.at[other if p else par, there])
    scores_of(
        jnp.concatenate([sinkb[0, 0:half], sinkb[1, 0:half]], 0),
        STEPS, jk < jnp.where(b >= 1, sink_end, 0),
    )

    total = STEPS + 1
    top_score = jnp.max(st[0], axis=0, keepdims=True)
    for i in range(1, total):
        top_score = jnp.maximum(top_score, jnp.max(st[i], axis=0, keepdims=True))
    norm = jnp.zeros((1, rows), f32)
    for i in range(total):
        e = jnp.exp(st[i] - top_score)
        st[i] = e
        norm = norm + jnp.sum(e, axis=0, keepdims=True)
    scale = 1.0 / norm
    w = 2 * half

    def parted(grad):
        low, high = grad[0:half], grad[half:]
        return jnp.where(par == 0, low, high), jnp.where(par == 0, high, low)

    def value_grad(i):
        probs = st[i] * scale
        st[i] = probs
        hi, lo = two(probs)
        both = dot(hi, gcat[:, 0:2 * w], NN)
        return parted((both[:, 0:w] + both[:, w:] + dot(lo, gcat[:, 0:w], NN)).T)

    def far_grad(kind, keep, give):
        g4out[kind, 0] = keep
        g4out[kind, 1] = give
        start(f"g4k{kind}", g4out.at[kind, 0], g4in.at[kind, 0], seq(-FAR))
        start(f"g4g{kind}", g4out.at[kind, 1], g4in.at[kind, 1], seq(-FAR))

    def near_grad(kind, o, keep, give):
        mine[kind, o] = keep
        xout[kind, o] = give
        start(f"gx{o}{kind}", xout.at[kind, o], xin.at[kind, o], across)

    def own_grad(kind, keep, give):
        arrived(f"g4g{kind}", g4in.at[kind, 1])
        near_grad(kind, 0, keep, give + g4in[kind, 1])

    def pass_on(kind, o):
        arrived(f"gx{o}{kind}", xin.at[kind, o])
        gout[kind, o] = mine[kind, o] + xin[kind, o]
        start(f"gz{o}{kind}", gout.at[kind, o], gin.at[kind, o], seq(-o))

    near = list(range(FAR - 1, 0, -1))
    for o in near:
        near_grad(1, o, *value_grad(o))
    far_grad(1, *value_grad(FAR))
    sg[0, half:w], sg[1, half:w] = value_grad(STEPS)

    delta = jnp.zeros((1, rows), f32)

    def weigh(i, delta):
        return delta + jnp.sum(st[i] * dp[i], axis=0, keepdims=True)

    products_of(jnp.concatenate([sinkb[0, half:], sinkb[1, half:]], 0), STEPS)
    delta = weigh(STEPS, delta)
    arrived(f"w{FAR}1", buf.at[1, FAR, par])
    arrived("w4x1", buf.at[1, FAR, other])
    products_of(joined(1, FAR), FAR)
    delta = weigh(FAR, delta)
    pass_on(1, FAR - 1)
    own_grad(1, *value_grad(0))
    products_of(joined(1, 0), 0)
    delta = weigh(0, delta)
    for o in range(1, FAR):
        arrived(f"r{o}1", buf.at[1, o, other])
        products_of(joined(1, o), o)
        delta = weigh(o, delta)
        if o < FAR - 1:
            pass_on(1, FAR - 1 - o)

    def key_grad(i):
        hi, lo = two(st[i] * (dp[i] - delta))
        dshi[i] = hi
        dslo[i] = lo
        both = dot(hi, qcat[:, 0:2 * w], NN)
        grad = temper * (both[:, 0:w] + both[:, w:] + dot(lo, qcat[:, 0:w], NN))
        return parted(grad.T)

    sg[0, 0:half], sg[1, 0:half] = key_grad(STEPS)
    for p, d in columns:
        target = lax.rem(inner + d, ni)
        rng = pl.ds(pl.multiple_of(target * pr, pr), pr)
        start(f"b1_{p}_{d}", sg.at[p, rng], sin.at[p * ni + d], column(p, d))

    for o in near:
        near_grad(0, o, *key_grad(o))
    far_grad(0, *key_grad(FAR))
    pass_on(0, near[0])
    keep, give = key_grad(0)
    own_grad(0, keep, give)
    for o in near[1:]:
        pass_on(0, o)

    for p, d in columns:
        arrived(f"b1_{p}_{d}", sin.at[p * ni + d])
    acc = sg[0, where]
    for p, d in columns:
        acc = acc + sin[p * ni + d]
    s2[...] = acc
    for z in range(1, no):
        @pl.when(outer == z)
        def _():
            copy(f"b2_{z}", s2, s2in.at[z], (head, inner, 0)).start()

    dqt = jnp.zeros((2 * half, rows), f32)
    for i in range(total):
        hi = dshi[i]
        dqt = dqt + dot(ktcat[i], jnp.concatenate([hi, hi, dslo[i]], 0), NN)
    dq_ref[...] = dqt.T

    @pl.when(top)
    def _():
        part = s2[...]
        for z in range(1, no):
            arrived(f"b2_{z}", s2in.at[z])
            part = part + s2in[z]
        s3[...] = part
        for i in range(1, ni):
            @pl.when(inner == i)
            def _():
                copy(f"b3_{i}", s3, s3in.at[i], (head, 0, outer)).start()

    for kind in range(1, -1, -1):
        arrived(f"g4k{kind}", g4in.at[kind, 0])
        arrived(f"gx0{kind}", xin.at[kind, 0])
        acc = mine[kind, 0] + g4in[kind, 0] + xin[kind, 0]
        for o in near:
            arrived(f"gz{o}{kind}", gin.at[kind, o])
            acc = acc + gin[kind, o]
        fin[kind * half:(kind + 1) * half] = acc

    @pl.when(first)
    def _():
        fin[0:pr] += s3[...]
        for i in range(1, ni):
            arrived(f"b3_{i}", s3in.at[i])
            fin[i * pr:(i + 1) * pr] += s3in[i]

    dkv_ref[...] = fin[...]

    for c in pending:
        c.wait_send()

    @pl.when(first)
    def _():
        for i in range(1, ni):
            copy(f"f1_{i}", own.at[pl.ds(i * pr, pr)], at_root, (head, i, outer)).wait_send()

    @pl.when(top)
    def _():
        for z in range(1, no):
            copy(f"f2_{z}", piece, piece, (head, inner, z)).wait_send()
        for i in range(1, ni):
            @pl.when(inner == i)
            def _():
                copy(f"b3_{i}", s3, s3in.at[i], (head, 0, outer)).wait_send()

    for z in range(1, no):
        @pl.when(outer == z)
        def _():
            copy(f"b2_{z}", s2, s2in.at[z], (head, inner, 0)).wait_send()
    assert len(slots) <= send.shape[0]


def store(dq_ref, dkv_ref, dq_hbm, dk_hbm, dv_hbm, sem):
    half = dk_hbm.shape[0]
    moves = [
        (dq_ref, dq_hbm), (dkv_ref.at[0:half], dk_hbm), (dkv_ref.at[half:2 * half], dv_hbm),
    ]
    copies = [pltpu.make_async_copy(x, y, sem.at[i]) for i, (x, y) in enumerate(moves)]
    for c in copies:
        c.start()
    for c in copies:
        c.wait()


def shards(ni, no, queries, key_rows, values, out_grad, sink_len, window_len, block_codes):
    block, heads_dev, dim = queries.shape
    rows = block * heads_dev
    half = key_rows.shape[1]
    codes = block_codes.T
    pr = block // ni
    total = STEPS + 1
    sems = 2 * (ni - 1) + 2 * (no - 1) + 2 * (2 * ni - 1) + 8 * STEPS
    smem = pl.BlockSpec(memory_space=pltpu.SMEM)
    vmem, hbm = pl.BlockSpec(memory_space=pltpu.VMEM), pl.BlockSpec(memory_space=pltpu.HBM)
    tile = (block, dim)
    grad_q, grad_kv = pl.pallas_call(
        functools.partial(kernel, (ni, no, heads_dev)),
        out_shape=(
            pltpu.VMEM((rows, dim), f32),
            pltpu.VMEM((2 * half, block), f32),
        ),
        in_specs=[smem] * 2 + [hbm] * 5,
        out_specs=(vmem,) * 2,
        scratch_shapes=[
            pltpu.SMEM(codes.shape, jnp.int32),
            pltpu.VMEM((rows, dim), f32),
            pltpu.VMEM((rows, dim), f32),
            pltpu.SemaphoreType.DMA((7,)),
            pltpu.VMEM(tile, f32),
            pltpu.VMEM((2, STEPS, 2, half, block), f32),
            pltpu.VMEM((2,) + tile, f32),
            pltpu.VMEM((pr, dim), f32),
            pltpu.VMEM((rows, 6 * dim), bf16),
            pltpu.VMEM((rows, 6 * dim), bf16),
            pltpu.VMEM((total, block, rows), f32),
            pltpu.VMEM((total, block, rows), f32),
            pltpu.VMEM((total, block, rows), bf16),
            pltpu.VMEM((total, block, rows), bf16),
            pltpu.VMEM((total, dim, 3 * block), bf16),
            pltpu.VMEM((2, FAR, half, block), f32),
            pltpu.VMEM((2, FAR, half, block), f32),
            pltpu.VMEM((2, FAR, half, block), f32),
            pltpu.VMEM((2, FAR, half, block), f32),
            pltpu.VMEM((2, FAR, half, block), f32),
            pltpu.VMEM((2, 2, half, block), f32),
            pltpu.VMEM((2, 2, half, block), f32),
            pltpu.VMEM(tile, f32),
            pltpu.VMEM((2,) + tile, f32),
            pltpu.VMEM((2 * ni, pr, dim), f32),
            pltpu.VMEM((pr, dim), f32),
            pltpu.VMEM((no, pr, dim), f32),
            pltpu.VMEM((pr, dim), f32),
            pltpu.VMEM((ni, pr, dim), f32),
            pltpu.SemaphoreType.DMA((sems,)),
            pltpu.SemaphoreType.DMA((sems,)),
        ],
        compiler_params=pltpu.CompilerParams(
            collective_id=0, has_side_effects=True, vmem_limit_bytes=66_000_000
        ),
    )(
        sink_len, window_len, codes,
        queries.reshape(rows, dim), key_rows.T, values.T, out_grad.reshape(rows, dim),
    )
    grad_q, grad_k, grad_v = pl.pallas_call(
        store,
        out_shape=(
            jax.ShapeDtypeStruct((rows, dim), f32),
            jax.ShapeDtypeStruct((half, block), f32),
            jax.ShapeDtypeStruct((half, block), f32),
        ),
        in_specs=[vmem] * 2,
        out_specs=(hbm,) * 3,
        scratch_shapes=[pltpu.SemaphoreType.DMA((3,))],
        compiler_params=pltpu.CompilerParams(vmem_limit_bytes=1 << 20),
    )(grad_q, grad_kv)
    return grad_q.reshape(queries.shape), grad_k.T, grad_v.T


def solution(mesh):
    in_specs = (
        P(("inner", "outer"), "head", None),
        P(("inner", "outer"), "head"),
        P(("inner", "outer"), "head"),
        P(("inner", "outer"), "head", None),
        P(),
        P(),
        P(),
    )
    out_specs = (
        P(("inner", "outer"), "head", None),
        P(("inner", "outer"), "head"),
        P(("inner", "outer"), "head"),
    )
    body = functools.partial(shards, mesh.shape["inner"], mesh.shape["outer"])
    return jax.shard_map(body, mesh=mesh, in_specs=in_specs, out_specs=out_specs, check_vma=False)
```

```python
import functools
import math

import jax
import jax.numpy as jnp
from jax import lax
from jax.experimental import pallas as pl
from jax.experimental.pallas import tpu as pltpu
from jax.sharding import PartitionSpec as P

STEPS = 5
FAR = STEPS - 1
BIG = 1 << 28
very_low = -1e30
f32, bf16 = jnp.float32, jnp.bfloat16
MESH = pl.DeviceIdType.MESH
NT = (((1,), (1,)), ((), ()))
NN = (((1,), (0,)), ((), ()))


def dot(a, b, dims):
    return lax.dot_general(a, b, dims, preferred_element_type=f32)


def two(x):
    hi = x.astype(bf16)
    return hi, (x - hi.astype(f32)).astype(bf16)


def three(x):
    hi = x.astype(bf16)
    rest = x - hi.astype(f32)
    mid = rest.astype(bf16)
    return hi, mid, (rest - mid.astype(f32)).astype(bf16)


def kernel(
    sizes, limits_ref, codes_hbm, q_hbm, k_hbm, v_hbm, g_hbm, dq_ref, dkv_ref,
    codes_ref, q_ref, g_ref, load, buf, sinkb, piece, qcat, gcat, st, dp, dshi, dslo, ktcat,
    xout, xin, mine, gout, gin, g4out, g4in, sg, sin, s2, s2in, s3, s3in, send, recv,
):
    ni, no, heads_dev = sizes
    half, block = k_hbm.shape
    rows = q_ref.shape[0]
    temper = 1.0 / math.sqrt(2 * half)
    head, inner, outer = lax.axis_index("head"), lax.axis_index("inner"), lax.axis_index("outer")
    par = lax.rem(head, 2)
    other = 1 - par
    partner = head + 1 - 2 * par
    count = ni * no
    b = inner * no + outer
    pr = block // ni

    def seq(o):
        t = lax.rem(b + o + count, count)
        return (head, t // no, lax.rem(t, no))

    across = (partner, inner, outer)
    columns = [(p, d) for p in range(2) for d in range(ni) if p or d]

    def column(p, d):
        return (partner if p else head, lax.rem(inner + d, ni), outer)

    def source(d):
        return lax.rem(inner - d + ni, ni)

    slots = {}

    def sem(name):
        return slots.setdefault(name, len(slots))

    pending = []

    def copy(name, src, dst, device):
        k = sem(name)
        return pltpu.make_async_remote_copy(
            src_ref=src, dst_ref=dst, send_sem=send.at[k], recv_sem=recv.at[k],
            device_id=device, device_id_type=MESH,
        )

    def start(name, src, dst, device):
        c = copy(name, src, dst, device)
        c.start()
        pending.append(c)

    def arrived(name, dst):
        copy(name, dst, dst, across).wait_recv()

    moves = [
        (k_hbm, buf.at[0, par, 0:half]), (v_hbm, buf.at[0, par, half:2 * half]),
        (q_hbm, q_ref), (g_hbm, g_ref),
        (codes_hbm, codes_ref),
    ]
    loads = [pltpu.make_async_copy(x, y, load.at[i]) for i, (x, y) in enumerate(moves)]
    for x in loads:
        x.start()

    barrier = pltpu.get_barrier_semaphore()
    greet = [seq(s * o) for o in range(1, STEPS) for s in (1, -1)]
    greet += [column(p, d) for p, d in columns]
    greet += [(head, inner, lax.rem(outer + d, no)) for d in range(1, no)]
    for device in greet:
        pl.semaphore_signal(barrier, inc=1, device_id=device, device_id_type=MESH)

    for x in loads:
        x.wait()
    q0, q1, q2 = three(q_ref[...])
    qcat[...] = jnp.concatenate([q0, q1, q0, q1, q2, q0], 1)
    g0, g1, g2 = three(g_ref[...])
    gcat[...] = jnp.concatenate([g0, g1, g0, g1, g2, g0], 1)
    pl.semaphore_wait(barrier, len(greet))

    own = buf.at[0, par]
    first = (inner == 0) & (outer == 0)
    top = outer == 0
    at_root = piece

    @pl.when(first)
    def _():
        for i in range(1, ni):
            copy(f"f1_{i}", own.at[pl.ds(i * pr, pr)], at_root, (head, i, outer)).start()
        piece[...] = buf[0, par, 0:pr, :]

    start("x0", own, own, across)
    for o in range(FAR, 0, -1):
        start(f"w{o}", own, buf.at[o, par], seq(o))

    def scores_of(a, c, index, allowed):
        keys = jnp.concatenate([a[0:half], c[0:half]], 0)
        vals = jnp.concatenate([a[half:], c[half:]], 0)
        k0, k1, k2 = three(keys.T)
        v0, v1, v2 = three(vals.T)
        s = dot(jnp.concatenate([k0, k0, k1, k1, k0, k2], 1), qcat[...], NT)
        st[index] = jnp.where(allowed, temper * s, very_low)
        dp[index] = dot(jnp.concatenate([v0, v0, v1, v1, v0, v2], 1), gcat[...], NT)
        t0, t1 = two(keys * temper)
        ktcat[index] = jnp.concatenate([t0, t1, t0], 1)

    jk = lax.broadcasted_iota(jnp.int32, (block, rows), 0)
    iq = lax.broadcasted_iota(jnp.int32, (block, rows), 1) // heads_dev
    gap = iq - jk
    sink_end, window = limits_ref[0], limits_ref[1]

    def mask_of(o):
        code = codes_ref[o, b]
        limit = jnp.where(code == 2, BIG, jnp.where(code == 1, window, -BIG))
        limit = jnp.where(b >= o, limit, -BIG) - o * block
        here = jnp.where(b == o, sink_end, 0)
        if o == 0:
            return (gap >= 0) & ((gap < limit) | (jk < here))
        return (gap < limit) & (jk >= here)

    def slot(o):
        scores_of(buf[o, 0], buf[o, 1], o, mask_of(o))

    arrived("x0", buf.at[0, other])
    start("w4x", buf.at[0, other], buf.at[FAR, other], seq(FAR))

    @pl.when(top)
    def _():
        @pl.when(inner != 0)
        def _():
            for i in range(1, ni):
                @pl.when(inner == i)
                def _():
                    arrived(f"f1_{i}", piece)
        for z in range(1, no):
            copy(f"f2_{z}", piece, piece, (head, inner, z)).start()

    slot(0)
    def relay(order):
        for o in order:
            arrived(f"w{o}", buf.at[o, par])
            copy(f"r{o}", buf.at[o, par], buf.at[o, par], across).start()

    up = list(range(1, FAR))

    @pl.when(outer == 0)
    def _():
        relay(up[::-1])

    @pl.when(outer == no - 1)
    def _():
        relay(up)

    @pl.when((outer != 0) & (outer != no - 1))
    def _():
        relay(up[::2] + up[1::2])

    for o in up:
        pending.append(copy(f"r{o}", buf.at[o, par], buf.at[o, par], across))

    @pl.when(outer != 0)
    def _():
        for z in range(1, no):
            @pl.when(outer == z)
            def _():
                arrived(f"f2_{z}", piece)

    where = pl.ds(pl.multiple_of(inner * pr, pr), pr)
    for p, d in columns:
        start(f"f3_{p}_{d}", piece, sinkb.at[par, where], column(p, d))
    sinkb[par, where] = piece[...]

    arrived(f"w{FAR}", buf.at[FAR, par])
    arrived("w4x", buf.at[FAR, other])
    slot(FAR)
    for o in range(1, FAR):
        arrived(f"r{o}", buf.at[o, other])
        slot(o)
    for p, d in columns:
        there = pl.ds(pl.multiple_of(source(d) * pr, pr), pr)
        arrived(f"f3_{p}_{d}", sinkb.at[other if p else par, there])
    scores_of(sinkb[0], sinkb[1], STEPS, jk < jnp.where(b >= 1, sink_end, 0))

    total = STEPS + 1
    top_score = jnp.max(st[0], axis=0, keepdims=True)
    for i in range(1, total):
        top_score = jnp.maximum(top_score, jnp.max(st[i], axis=0, keepdims=True))
    norm = jnp.zeros((1, rows), f32)
    delta = jnp.zeros((1, rows), f32)
    for i in range(total):
        e = jnp.exp(st[i] - top_score)
        st[i] = e
        norm = norm + jnp.sum(e, axis=0, keepdims=True)
        delta = delta + jnp.sum(e * dp[i], axis=0, keepdims=True)
    scale = 1.0 / norm
    delta = delta * scale

    def grads(i):
        probs = st[i] * scale
        ds = probs * (dp[i] - delta)
        p_hi, p_lo = two(probs)
        d_hi, d_lo = two(ds)
        dshi[i] = d_hi
        dslo[i] = d_lo
        w = 2 * half
        pv = dot(p_hi, gcat[:, 0:2 * w], NN)
        dv = pv[:, 0:w] + pv[:, w:] + dot(p_lo, gcat[:, 0:w], NN)
        kq = dot(d_hi, qcat[:, 0:2 * w], NN)
        dk = temper * (kq[:, 0:w] + kq[:, w:] + dot(d_lo, qcat[:, 0:w], NN))
        dk, dv = dk.T, dv.T
        even = jnp.concatenate([dk[0:half], dv[0:half]], 0)
        odd = jnp.concatenate([dk[half:], dv[half:]], 0)
        keep = jnp.where(par == 0, even, odd)
        give = jnp.where(par == 0, odd, even)
        return keep, give

    def pass_on(o):
        arrived(f"gx{o}", xin.at[o])
        gout[o] = mine[o] + xin[o]
        start(f"gz{o}", gout.at[o], gin.at[o], seq(-o))

    def near(o):
        keep, give = grads(o)
        mine[o] = keep
        xout[o] = give
        start(f"gx{o}", xout.at[o], xin.at[o], across)

    near(FAR - 1)
    keep, give = grads(STEPS)
    sg[0] = keep
    sg[1] = give
    for p, d in columns:
        target = lax.rem(inner + d, ni)
        rng = pl.ds(pl.multiple_of(target * pr, pr), pr)
        start(f"b1_{p}_{d}", sg.at[p, rng], sin.at[p * ni + d], column(p, d))

    near(FAR - 2)
    pass_on(FAR - 1)
    keep, give = grads(FAR)
    g4out[0] = keep
    g4out[1] = give
    start("g4k", g4out.at[0], g4in.at[0], seq(-FAR))
    start("g4g", g4out.at[1], g4in.at[1], seq(-FAR))

    for o in range(FAR - 3, 0, -1):
        near(o)
        pass_on(o + 1)
    for p, d in columns:
        arrived(f"b1_{p}_{d}", sin.at[p * ni + d])
    acc = sg[0, where]
    for p, d in columns:
        acc = acc + sin[p * ni + d]
    s2[...] = acc
    for z in range(1, no):
        @pl.when(outer == z)
        def _():
            copy(f"b2_{z}", s2, s2in.at[z], (head, inner, 0)).start()

    keep, give = grads(0)
    arrived("g4g", g4in.at[1])
    xout[0] = give + g4in[1]
    start("gx0", xout.at[0], xin.at[0], across)
    pass_on(1)
    arrived("g4k", g4in.at[0])
    mine[0] = keep + g4in[0]

    dqt = jnp.zeros((2 * half, rows), f32)
    for i in range(total):
        hi = dshi[i]
        dqt = dqt + dot(ktcat[i], jnp.concatenate([hi, hi, dslo[i]], 0), NN)
    dq_ref[...] = dqt.T

    @pl.when(top)
    def _():
        part = s2[...]
        for z in range(1, no):
            arrived(f"b2_{z}", s2in.at[z])
            part = part + s2in[z]
        s3[...] = part
        for i in range(1, ni):
            @pl.when(inner == i)
            def _():
                copy(f"b3_{i}", s3, s3in.at[i], (head, 0, outer)).start()

    arrived("gx0", xin.at[0])
    acc = mine[0] + xin[0]
    for o in range(FAR - 1, 0, -1):
        arrived(f"gz{o}", gin.at[o])
        acc = acc + gin[o]
    mine[0] = acc

    @pl.when(first)
    def _():
        mine[0, 0:pr] += s3[...]
        for i in range(1, ni):
            arrived(f"b3_{i}", s3in.at[i])
            mine[0, i * pr:(i + 1) * pr] += s3in[i]

    dkv_ref[...] = mine[0]

    for c in pending:
        c.wait_send()

    @pl.when(first)
    def _():
        for i in range(1, ni):
            copy(f"f1_{i}", own.at[pl.ds(i * pr, pr)], at_root, (head, i, outer)).wait_send()

    @pl.when(top)
    def _():
        for z in range(1, no):
            copy(f"f2_{z}", piece, piece, (head, inner, z)).wait_send()
        for i in range(1, ni):
            @pl.when(inner == i)
            def _():
                copy(f"b3_{i}", s3, s3in.at[i], (head, 0, outer)).wait_send()

    for z in range(1, no):
        @pl.when(outer == z)
        def _():
            copy(f"b2_{z}", s2, s2in.at[z], (head, inner, 0)).wait_send()
    assert len(slots) <= send.shape[0]


def store(dq_ref, dkv_ref, dq_hbm, dk_hbm, dv_hbm, sem):
    half = dk_hbm.shape[0]
    moves = [
        (dq_ref, dq_hbm), (dkv_ref.at[0:half], dk_hbm), (dkv_ref.at[half:2 * half], dv_hbm),
    ]
    copies = [pltpu.make_async_copy(x, y, sem.at[i]) for i, (x, y) in enumerate(moves)]
    for c in copies:
        c.start()
    for c in copies:
        c.wait()


def shards(ni, no, queries, key_rows, values, out_grad, sink_len, window_len, block_codes):
    block, heads_dev, dim = queries.shape
    rows = block * heads_dev
    half = key_rows.shape[1]
    codes = block_codes.T
    pr = block // ni
    total = STEPS + 1
    sems = 2 * (ni - 1) + 2 * (no - 1) + 2 * (2 * ni - 1) + 4 * STEPS
    smem = pl.BlockSpec(memory_space=pltpu.SMEM)
    vmem, hbm = pl.BlockSpec(memory_space=pltpu.VMEM), pl.BlockSpec(memory_space=pltpu.HBM)
    tile = (block, dim)
    grad_q, grad_kv = pl.pallas_call(
        functools.partial(kernel, (ni, no, heads_dev)),
        out_shape=(
            pltpu.VMEM((rows, dim), f32),
            pltpu.VMEM((2 * half, block), f32),
        ),
        in_specs=[smem] + [hbm] * 5,
        out_specs=(vmem,) * 2,
        scratch_shapes=[
            pltpu.SMEM(codes.shape, jnp.int32),
            pltpu.VMEM((rows, dim), f32),
            pltpu.VMEM((rows, dim), f32),
            pltpu.SemaphoreType.DMA((5,)),
            pltpu.VMEM((STEPS, 2) + tile, f32),
            pltpu.VMEM((2,) + tile, f32),
            pltpu.VMEM((pr, dim), f32),
            pltpu.VMEM((rows, 6 * dim), bf16),
            pltpu.VMEM((rows, 6 * dim), bf16),
            pltpu.VMEM((total, block, rows), f32),
            pltpu.VMEM((total, block, rows), f32),
            pltpu.VMEM((total, block, rows), bf16),
            pltpu.VMEM((total, block, rows), bf16),
            pltpu.VMEM((total, dim, 3 * block), bf16),
            pltpu.VMEM((FAR,) + tile, f32),
            pltpu.VMEM((FAR,) + tile, f32),
            pltpu.VMEM((FAR,) + tile, f32),
            pltpu.VMEM((FAR,) + tile, f32),
            pltpu.VMEM((FAR,) + tile, f32),
            pltpu.VMEM((2,) + tile, f32),
            pltpu.VMEM((2,) + tile, f32),
            pltpu.VMEM((2,) + tile, f32),
            pltpu.VMEM((2 * ni, pr, dim), f32),
            pltpu.VMEM((pr, dim), f32),
            pltpu.VMEM((no, pr, dim), f32),
            pltpu.VMEM((pr, dim), f32),
            pltpu.VMEM((ni, pr, dim), f32),
            pltpu.SemaphoreType.DMA((sems,)),
            pltpu.SemaphoreType.DMA((sems,)),
        ],
        compiler_params=pltpu.CompilerParams(
            collective_id=0, has_side_effects=True, vmem_limit_bytes=66_000_000
        ),
    )(
        jnp.concatenate([sink_len, window_len]), codes,
        queries.reshape(rows, dim), key_rows.T, values.T, out_grad.reshape(rows, dim),
    )
    grad_q, grad_k, grad_v = pl.pallas_call(
        store,
        out_shape=(
            jax.ShapeDtypeStruct((rows, dim), f32),
            jax.ShapeDtypeStruct((half, block), f32),
            jax.ShapeDtypeStruct((half, block), f32),
        ),
        in_specs=[vmem] * 2,
        out_specs=(hbm,) * 3,
        scratch_shapes=[pltpu.SemaphoreType.DMA((3,))],
        compiler_params=pltpu.CompilerParams(vmem_limit_bytes=1 << 20),
    )(grad_q, grad_kv)
    return grad_q.reshape(queries.shape), grad_k.T, grad_v.T


def solution(mesh):
    in_specs = (
        P(("inner", "outer"), "head", None),
        P(("inner", "outer"), "head"),
        P(("inner", "outer"), "head"),
        P(("inner", "outer"), "head", None),
        P(),
        P(),
        P(),
    )
    out_specs = (
        P(("inner", "outer"), "head", None),
        P(("inner", "outer"), "head"),
        P(("inner", "outer"), "head"),
    )
    body = functools.partial(shards, mesh.shape["inner"], mesh.shape["outer"])
    return jax.shard_map(body, mesh=mesh, in_specs=in_specs, out_specs=out_specs, check_vma=False)
```

```python
import functools
import math

import jax
import jax.numpy as jnp
from jax import lax
from jax.experimental import pallas as pl
from jax.experimental.pallas import tpu as pltpu
from jax.sharding import PartitionSpec as P

STEPS = 5
FAR = STEPS - 1
BIG = 1 << 28
very_low = -1e30
f32, bf16 = jnp.float32, jnp.bfloat16
MESH = pl.DeviceIdType.MESH
NT = (((1,), (1,)), ((), ()))
NN = (((1,), (0,)), ((), ()))


def dot(a, b, dims):
    return lax.dot_general(a, b, dims, preferred_element_type=f32)


def two(x):
    hi = x.astype(bf16)
    return hi, (x - hi.astype(f32)).astype(bf16)


def three(x):
    hi = x.astype(bf16)
    rest = x - hi.astype(f32)
    mid = rest.astype(bf16)
    return hi, mid, (rest - mid.astype(f32)).astype(bf16)


def kernel(
    sizes, sink_ref, window_ref, codes_hbm, q_hbm, k_hbm, v_hbm, g_hbm, dq_ref, dkv_ref,
    codes_ref, q_ref, g_ref, load, buf, sinkb, piece, qcat, gcat, st, dp, dshi, dslo, ktcat,
    xout, xin, mine, gout, gin, g4out, g4in, sg, sin, s2, s2in, s3, s3in, send, recv,
):
    ni, no, heads_dev = sizes
    half, block = k_hbm.shape
    rows = q_ref.shape[0]
    temper = 1.0 / math.sqrt(2 * half)
    head, inner, outer = lax.axis_index("head"), lax.axis_index("inner"), lax.axis_index("outer")
    par = lax.rem(head, 2)
    other = 1 - par
    partner = head + 1 - 2 * par
    count = ni * no
    b = inner * no + outer
    pr = block // ni

    def seq(o):
        t = lax.rem(b + o + count, count)
        return (head, t // no, lax.rem(t, no))

    across = (partner, inner, outer)
    columns = [(p, d) for p in range(2) for d in range(ni) if p or d]

    def column(p, d):
        return (partner if p else head, lax.rem(inner + d, ni), outer)

    def source(d):
        return lax.rem(inner - d + ni, ni)

    slots = {}

    def sem(name):
        return slots.setdefault(name, len(slots))

    pending = []

    def copy(name, src, dst, device):
        k = sem(name)
        return pltpu.make_async_remote_copy(
            src_ref=src, dst_ref=dst, send_sem=send.at[k], recv_sem=recv.at[k],
            device_id=device, device_id_type=MESH,
        )

    def start(name, src, dst, device):
        c = copy(name, src, dst, device)
        c.start()
        pending.append(c)

    def arrived(name, dst):
        copy(name, dst, dst, across).wait_recv()

    moves = [
        (k_hbm, buf.at[0, par, 0:half]), (v_hbm, buf.at[0, par, half:2 * half]),
        (q_hbm, q_ref), (g_hbm, g_ref),
        (codes_hbm, codes_ref),
    ]
    loads = [pltpu.make_async_copy(x, y, load.at[i]) for i, (x, y) in enumerate(moves)]
    for x in loads:
        x.start()

    barrier = pltpu.get_barrier_semaphore()
    greet = [seq(s * o) for o in range(1, STEPS) for s in (1, -1)]
    greet += [column(p, d) for p, d in columns]
    greet += [(head, inner, lax.rem(outer + d, no)) for d in range(1, no)]
    for device in greet:
        pl.semaphore_signal(barrier, inc=1, device_id=device, device_id_type=MESH)

    for x in loads:
        x.wait()
    q0, q1, q2 = three(q_ref[...])
    qcat[...] = jnp.concatenate([q0, q1, q0, q1, q2, q0], 1)
    g0, g1, g2 = three(g_ref[...])
    gcat[...] = jnp.concatenate([g0, g1, g0, g1, g2, g0], 1)
    pl.semaphore_wait(barrier, len(greet))

    own = buf.at[0, par]
    first = (inner == 0) & (outer == 0)
    top = outer == 0
    at_root = piece

    @pl.when(first)
    def _():
        for i in range(1, ni):
            copy(f"f1_{i}", own.at[pl.ds(i * pr, pr)], at_root, (head, i, outer)).start()
        piece[...] = buf[0, par, 0:pr, :]

    start("x0", own, own, across)
    for o in range(FAR, 0, -1):
        start(f"w{o}", own, buf.at[o, par], seq(o))

    def scores_of(a, c, index, allowed):
        keys = jnp.concatenate([a[0:half], c[0:half]], 0)
        vals = jnp.concatenate([a[half:], c[half:]], 0)
        k0, k1, k2 = three(keys.T)
        v0, v1, v2 = three(vals.T)
        s = dot(jnp.concatenate([k0, k0, k1, k1, k0, k2], 1), qcat[...], NT)
        st[index] = jnp.where(allowed, temper * s, very_low)
        dp[index] = dot(jnp.concatenate([v0, v0, v1, v1, v0, v2], 1), gcat[...], NT)
        t0, t1 = two(keys * temper)
        ktcat[index] = jnp.concatenate([t0, t1, t0], 1)

    jk = lax.broadcasted_iota(jnp.int32, (block, rows), 0)
    iq = lax.broadcasted_iota(jnp.int32, (block, rows), 1) // heads_dev
    gap = iq - jk
    sink_end, window = sink_ref[0], window_ref[0]

    def mask_of(o):
        code = codes_ref[o, b]
        limit = jnp.where(code == 2, BIG, jnp.where(code == 1, window, -BIG))
        limit = jnp.where(b >= o, limit, -BIG) - o * block
        here = jnp.where(b == o, sink_end, 0)
        if o == 0:
            return (gap >= 0) & ((gap < limit) | (jk < here))
        return (gap < limit) & (jk >= here)

    def slot(o):
        scores_of(buf[o, 0], buf[o, 1], o, mask_of(o))

    arrived("x0", buf.at[0, other])
    start("w4x", buf.at[0, other], buf.at[FAR, other], seq(FAR))

    @pl.when(top)
    def _():
        @pl.when(inner != 0)
        def _():
            for i in range(1, ni):
                @pl.when(inner == i)
                def _():
                    arrived(f"f1_{i}", piece)
        for z in range(1, no):
            copy(f"f2_{z}", piece, piece, (head, inner, z)).start()

    slot(0)
    def relay(order):
        for o in order:
            arrived(f"w{o}", buf.at[o, par])
            copy(f"r{o}", buf.at[o, par], buf.at[o, par], across).start()

    up = list(range(1, FAR))

    @pl.when(outer == 0)
    def _():
        relay(up[::-1])

    @pl.when(outer == no - 1)
    def _():
        relay(up)

    @pl.when((outer != 0) & (outer != no - 1))
    def _():
        relay(up[::2] + up[1::2])

    for o in up:
        pending.append(copy(f"r{o}", buf.at[o, par], buf.at[o, par], across))

    @pl.when(outer != 0)
    def _():
        for z in range(1, no):
            @pl.when(outer == z)
            def _():
                arrived(f"f2_{z}", piece)

    where = pl.ds(pl.multiple_of(inner * pr, pr), pr)
    for p, d in columns:
        start(f"f3_{p}_{d}", piece, sinkb.at[par, where], column(p, d))
    sinkb[par, where] = piece[...]

    arrived(f"w{FAR}", buf.at[FAR, par])
    arrived("w4x", buf.at[FAR, other])
    slot(FAR)
    for o in range(1, FAR):
        arrived(f"r{o}", buf.at[o, other])
        slot(o)
    for p, d in columns:
        there = pl.ds(pl.multiple_of(source(d) * pr, pr), pr)
        arrived(f"f3_{p}_{d}", sinkb.at[other if p else par, there])
    scores_of(sinkb[0], sinkb[1], STEPS, jk < jnp.where(b >= 1, sink_end, 0))

    total = STEPS + 1
    top_score = jnp.max(st[0], axis=0, keepdims=True)
    for i in range(1, total):
        top_score = jnp.maximum(top_score, jnp.max(st[i], axis=0, keepdims=True))
    norm = jnp.zeros((1, rows), f32)
    delta = jnp.zeros((1, rows), f32)
    for i in range(total):
        e = jnp.exp(st[i] - top_score)
        st[i] = e
        norm = norm + jnp.sum(e, axis=0, keepdims=True)
        delta = delta + jnp.sum(e * dp[i], axis=0, keepdims=True)
    scale = 1.0 / norm
    delta = delta * scale

    def grads(i):
        probs = st[i] * scale
        ds = probs * (dp[i] - delta)
        p_hi, p_lo = two(probs)
        d_hi, d_lo = two(ds)
        dshi[i] = d_hi
        dslo[i] = d_lo
        w = 2 * half
        pv = dot(p_hi, gcat[:, 0:2 * w], NN)
        dv = pv[:, 0:w] + pv[:, w:] + dot(p_lo, gcat[:, 0:w], NN)
        kq = dot(d_hi, qcat[:, 0:2 * w], NN)
        dk = temper * (kq[:, 0:w] + kq[:, w:] + dot(d_lo, qcat[:, 0:w], NN))
        dk, dv = dk.T, dv.T
        even = jnp.concatenate([dk[0:half], dv[0:half]], 0)
        odd = jnp.concatenate([dk[half:], dv[half:]], 0)
        keep = jnp.where(par == 0, even, odd)
        give = jnp.where(par == 0, odd, even)
        return keep, give

    def pass_on(o):
        arrived(f"gx{o}", xin.at[o])
        gout[o] = mine[o] + xin[o]
        start(f"gz{o}", gout.at[o], gin.at[o], seq(-o))

    def near(o):
        keep, give = grads(o)
        mine[o] = keep
        xout[o] = give
        start(f"gx{o}", xout.at[o], xin.at[o], across)

    keep, give = grads(STEPS)
    sg[0] = keep
    sg[1] = give
    for p, d in columns:
        target = lax.rem(inner + d, ni)
        rng = pl.ds(pl.multiple_of(target * pr, pr), pr)
        start(f"b1_{p}_{d}", sg.at[p, rng], sin.at[p * ni + d], column(p, d))

    near(FAR - 1)
    near(FAR - 2)
    pass_on(FAR - 1)
    keep, give = grads(FAR)
    g4out[0] = keep
    g4out[1] = give
    start("g4k", g4out.at[0], g4in.at[0], seq(-FAR))
    start("g4g", g4out.at[1], g4in.at[1], seq(-FAR))

    for o in range(FAR - 3, 0, -1):
        near(o)
        pass_on(o + 1)
    for p, d in columns:
        arrived(f"b1_{p}_{d}", sin.at[p * ni + d])
    acc = sg[0, where]
    for p, d in columns:
        acc = acc + sin[p * ni + d]
    s2[...] = acc
    for z in range(1, no):
        @pl.when(outer == z)
        def _():
            copy(f"b2_{z}", s2, s2in.at[z], (head, inner, 0)).start()

    keep, give = grads(0)
    arrived("g4g", g4in.at[1])
    xout[0] = give + g4in[1]
    start("gx0", xout.at[0], xin.at[0], across)
    pass_on(1)
    arrived("g4k", g4in.at[0])
    mine[0] = keep + g4in[0]

    dqt = jnp.zeros((2 * half, rows), f32)
    for i in range(total):
        hi = dshi[i]
        dqt = dqt + dot(ktcat[i], jnp.concatenate([hi, hi, dslo[i]], 0), NN)
    dq_ref[...] = dqt.T

    @pl.when(top)
    def _():
        part = s2[...]
        for z in range(1, no):
            arrived(f"b2_{z}", s2in.at[z])
            part = part + s2in[z]
        s3[...] = part
        for i in range(1, ni):
            @pl.when(inner == i)
            def _():
                copy(f"b3_{i}", s3, s3in.at[i], (head, 0, outer)).start()

    arrived("gx0", xin.at[0])
    acc = mine[0] + xin[0]
    for o in range(FAR - 1, 0, -1):
        arrived(f"gz{o}", gin.at[o])
        acc = acc + gin[o]
    mine[0] = acc

    @pl.when(first)
    def _():
        mine[0, 0:pr] += s3[...]
        for i in range(1, ni):
            arrived(f"b3_{i}", s3in.at[i])
            mine[0, i * pr:(i + 1) * pr] += s3in[i]

    dkv_ref[...] = mine[0]

    for c in pending:
        c.wait_send()

    @pl.when(first)
    def _():
        for i in range(1, ni):
            copy(f"f1_{i}", own.at[pl.ds(i * pr, pr)], at_root, (head, i, outer)).wait_send()

    @pl.when(top)
    def _():
        for z in range(1, no):
            copy(f"f2_{z}", piece, piece, (head, inner, z)).wait_send()
        for i in range(1, ni):
            @pl.when(inner == i)
            def _():
                copy(f"b3_{i}", s3, s3in.at[i], (head, 0, outer)).wait_send()

    for z in range(1, no):
        @pl.when(outer == z)
        def _():
            copy(f"b2_{z}", s2, s2in.at[z], (head, inner, 0)).wait_send()
    assert len(slots) <= send.shape[0]


def store(dq_ref, dkv_ref, dq_hbm, dk_hbm, dv_hbm, sem):
    half = dk_hbm.shape[0]
    moves = [
        (dq_ref, dq_hbm), (dkv_ref.at[0:half], dk_hbm), (dkv_ref.at[half:2 * half], dv_hbm),
    ]
    copies = [pltpu.make_async_copy(x, y, sem.at[i]) for i, (x, y) in enumerate(moves)]
    for c in copies:
        c.start()
    for c in copies:
        c.wait()


def shards(ni, no, queries, key_rows, values, out_grad, sink_len, window_len, block_codes):
    block, heads_dev, dim = queries.shape
    rows = block * heads_dev
    half = key_rows.shape[1]
    codes = block_codes.T
    pr = block // ni
    total = STEPS + 1
    sems = 2 * (ni - 1) + 2 * (no - 1) + 2 * (2 * ni - 1) + 4 * STEPS
    smem = pl.BlockSpec(memory_space=pltpu.SMEM)
    vmem, hbm = pl.BlockSpec(memory_space=pltpu.VMEM), pl.BlockSpec(memory_space=pltpu.HBM)
    tile = (block, dim)
    grad_q, grad_kv = pl.pallas_call(
        functools.partial(kernel, (ni, no, heads_dev)),
        out_shape=(
            pltpu.VMEM((rows, dim), f32),
            pltpu.VMEM((2 * half, block), f32),
        ),
        in_specs=[smem] * 2 + [hbm] * 5,
        out_specs=(vmem,) * 2,
        scratch_shapes=[
            pltpu.SMEM(codes.shape, jnp.int32),
            pltpu.VMEM((rows, dim), f32),
            pltpu.VMEM((rows, dim), f32),
            pltpu.SemaphoreType.DMA((5,)),
            pltpu.VMEM((STEPS, 2) + tile, f32),
            pltpu.VMEM((2,) + tile, f32),
            pltpu.VMEM((pr, dim), f32),
            pltpu.VMEM((rows, 6 * dim), bf16),
            pltpu.VMEM((rows, 6 * dim), bf16),
            pltpu.VMEM((total, block, rows), f32),
            pltpu.VMEM((total, block, rows), f32),
            pltpu.VMEM((total, block, rows), bf16),
            pltpu.VMEM((total, block, rows), bf16),
            pltpu.VMEM((total, dim, 3 * block), bf16),
            pltpu.VMEM((FAR,) + tile, f32),
            pltpu.VMEM((FAR,) + tile, f32),
            pltpu.VMEM((FAR,) + tile, f32),
            pltpu.VMEM((FAR,) + tile, f32),
            pltpu.VMEM((FAR,) + tile, f32),
            pltpu.VMEM((2,) + tile, f32),
            pltpu.VMEM((2,) + tile, f32),
            pltpu.VMEM((2,) + tile, f32),
            pltpu.VMEM((2 * ni, pr, dim), f32),
            pltpu.VMEM((pr, dim), f32),
            pltpu.VMEM((no, pr, dim), f32),
            pltpu.VMEM((pr, dim), f32),
            pltpu.VMEM((ni, pr, dim), f32),
            pltpu.SemaphoreType.DMA((sems,)),
            pltpu.SemaphoreType.DMA((sems,)),
        ],
        compiler_params=pltpu.CompilerParams(
            collective_id=0, has_side_effects=True, vmem_limit_bytes=66_000_000
        ),
    )(
        sink_len, window_len, codes,
        queries.reshape(rows, dim), key_rows.T, values.T, out_grad.reshape(rows, dim),
    )
    grad_q, grad_k, grad_v = pl.pallas_call(
        store,
        out_shape=(
            jax.ShapeDtypeStruct((rows, dim), f32),
            jax.ShapeDtypeStruct((half, block), f32),
            jax.ShapeDtypeStruct((half, block), f32),
        ),
        in_specs=[vmem] * 2,
        out_specs=(hbm,) * 3,
        scratch_shapes=[pltpu.SemaphoreType.DMA((3,))],
        compiler_params=pltpu.CompilerParams(vmem_limit_bytes=1 << 20),
    )(grad_q, grad_kv)
    return grad_q.reshape(queries.shape), grad_k.T, grad_v.T


def solution(mesh):
    in_specs = (
        P(("inner", "outer"), "head", None),
        P(("inner", "outer"), "head"),
        P(("inner", "outer"), "head"),
        P(("inner", "outer"), "head", None),
        P(),
        P(),
        P(),
    )
    out_specs = (
        P(("inner", "outer"), "head", None),
        P(("inner", "outer"), "head"),
        P(("inner", "outer"), "head"),
    )
    body = functools.partial(shards, mesh.shape["inner"], mesh.shape["outer"])
    return jax.shard_map(body, mesh=mesh, in_specs=in_specs, out_specs=out_specs, check_vma=False)
```
